16 devices in a mesh: rep: 2 (over y, z), dp: 8 (over x, core).
Axes of the slice: x: 4, y: 2, z: 1, core: 2. Of those that a mesh axis runs over, the one named last changes fastest.
The devices are a block of a 4x4x8 slice.
Arguments:
- x: bfloat16 [16, 2048, 640], P(('rep', 'dp')), parts along dimension 0
- dy: bfloat16 [16, 2048, 640], P(('rep', 'dp')), parts along dimension 0
- wq: bfloat16 [2, 640, 1024], replicated
- wk: bfloat16 [2, 640, 128], replicated
- wv: bfloat16 [2, 640, 128], replicated
- wo: bfloat16 [2, 1024, 640], replicated
- w_gate: bfloat16 [2, 640, 3200], replicated
- w_up: bfloat16 [2, 640, 3200], replicated
- w_down: bfloat16 [2, 3200, 640], replicated
- m_wq: float32 [2, 640, 1024], P(None, 'dp')
- m_wk: float32 [2, 640, 128], P(None, 'dp')
- m_wv: float32 [2, 640, 128], P(None, 'dp')
- m_wo: float32 [2, 1024, 640], P(None, 'dp')
- m_w_gate: float32 [2, 640, 3200], P(None, 'dp')
- m_w_up: float32 [2, 640, 3200], P(None, 'dp')
- m_w_down: float32 [2, 3200, 640], P(None, 'dp')
- v_wq: float32 [2, 640, 1024], P(None, 'dp')
- v_wk: float32 [2, 640, 128], P(None, 'dp')
- v_wv: float32 [2, 640, 128], P(None, 'dp')
- v_wo: float32 [2, 1024, 640], P(None, 'dp')
- v_w_gate: float32 [2, 640, 3200], P(None, 'dp')
- v_w_up: float32 [2, 640, 3200], P(None, 'dp')
- v_w_down: float32 [2, 3200, 640], P(None, 'dp')
Outputs:
- output 1: bfloat16 [4, 640, 1024], P('rep'), parts along dimension 0
- output 2: bfloat16 [4, 640, 128], P('rep'), parts along dimension 0
- output 3: bfloat16 [4, 640, 128], P('rep'), parts along dimension 0
- output 4: bfloat16 [4, 1024, 640], P('rep'), parts along dimension 0
- output 5: bfloat16 [4, 640, 3200], P('rep'), parts along dimension 0
- output 6: bfloat16 [4, 640, 3200], P('rep'), parts along dimension 0
- output 7: bfloat16 [4, 3200, 640], P('rep'), parts along dimension 0
- output 8: float32 [4, 640, 1024], P('rep', 'dp'), parts along dimension 0
- output 9: float32 [4, 640, 128], P('rep', 'dp'), parts along dimension 0
- output 10: float32 [4, 640, 128], P('rep', 'dp'), parts along dimension 0
- output 11: float32 [4, 1024, 640], P('rep', 'dp'), parts along dimension 0
- output 12: float32 [4, 640, 3200], P('rep', 'dp'), parts along dimension 0
- output 13: float32 [4, 640, 3200], P('rep', 'dp'), parts along dimension 0
- output 14: float32 [4, 3200, 640], P('rep', 'dp'), parts along dimension 0
- output 15: float32 [4, 640, 1024], P('rep', 'dp'), parts along dimension 0
- output 16: float32 [4, 640, 128], P('rep', 'dp'), parts along dimension 0
- output 17: float32 [4, 640, 128], P('rep', 'dp'), parts along dimension 0
- output 18: float32 [4, 1024, 640], P('rep', 'dp'), parts along dimension 0
- output 19: float32 [4, 640, 3200], P('rep', 'dp'), parts along dimension 0
- output 20: float32 [4, 640, 3200], P('rep', 'dp'), parts along dimension 0
- output 21: float32 [4, 3200, 640], P('rep', 'dp'), parts along dimension 0
There are 2 independent parts. The reference program is written for one: setup_inputs(seed, part) draws one part's arguments, and reference() takes and returns one part's arrays. A program takes and returns all parts, laid end to end along the dimension named above; an argument that names none is the same for every part.
All inputs are finite; a program needn't handle non-finite values.
Results may differ from the reference program's by a relative error of at most 0.024.
Values are sent between devices in bfloat16 or wider.
A program may use at most 768 MiB of HBM per device.

```python
import jax
import jax.numpy as jnp
from jax import lax

SEQUENCES = 8
TOKENS = 2048
D = 640
HEADS = 8
KV_HEADS = 1
HEAD = 128
FF = 3200
LAYERS = 2
THETA = 10000
NAMES = ("wq", "wk", "wv", "wo", "w_gate", "w_up", "w_down")
SHAPES = {
    "wq": (LAYERS, D, HEADS * HEAD),
    "wk": (LAYERS, D, KV_HEADS * HEAD),
    "wv": (LAYERS, D, KV_HEADS * HEAD),
    "wo": (LAYERS, HEADS * HEAD, D),
    "w_gate": (LAYERS, D, FF),
    "w_up": (LAYERS, D, FF),
    "w_down": (LAYERS, FF, D),
}


def bump(key, n, height):
    away = (jnp.arange(n, dtype=jnp.int32) - jax.random.randint(key, (), 0, n, jnp.int32)) % n
    return jnp.where(away < n // 8, height, 1.0)


def together(key, own, strength):
    shared = jax.random.normal(key, own.shape[1:], jnp.float32)
    return (own + strength * shared) * lax.rsqrt(1 + strength * strength)


def setup_inputs(seed: int = 0, part: int = 0) -> dict:
    kx, kdy, ka, kb, kz, kf, kh, kl, *keys = jax.random.split(jax.random.key(seed), 8 + 3 * len(NAMES))
    kx, kdy, ka, kb = (jax.random.fold_in(k, part) for k in (kx, kdy, ka, kb))
    kw, km, kv = (keys[i::3] for i in range(3))
    shape = (SEQUENCES, TOKENS, D)
    much_x, much_dy = jax.random.uniform(kz, (2,), jnp.float32, 0.0, 1.0)
    loud = 2.0 ** jax.random.uniform(jax.random.fold_in(kz, 1), (), jnp.float32, -1.0, 2.0)
    layers = 2.0 ** jax.random.uniform(kl, (LAYERS, 1, 1), jnp.float32, -1.0, 1.0)
    times = {"wq": 1.0, "wk": 1.0, "wv": 2.0, "wo": layers, "w_gate": 1.0, "w_up": bump(kh, FF, 4.0), "w_down": layers}
    x = together(ka, jax.random.normal(kx, shape, jnp.float32), much_x) * bump(kf, D, 4.0)
    dy = together(kb, jax.random.normal(kdy, shape, jnp.float32), much_dy)
    drawn = {"x": x.astype(jnp.bfloat16), "dy": (loud * dy * (SEQUENCES * TOKENS) ** -0.5).astype(jnp.bfloat16)}
    for key, name in zip(kw, NAMES, strict=True):
        drawn[name] = (jax.random.normal(key, SHAPES[name], jnp.float32) * SHAPES[name][1] ** -0.5 * times[name]).astype(jnp.bfloat16)
    for key, name in zip(km, NAMES, strict=True):
        drawn[f"m_{name}"] = 0.1 * jax.random.normal(key, SHAPES[name], jnp.float32)
    for key, name in zip(kv, NAMES, strict=True):
        drawn[f"v_{name}"] = loud * loud * jax.random.uniform(key, SHAPES[name], jnp.float32, 0.2, 0.6)
    return drawn


def matmul(a, w):
    return jnp.dot(a, w, preferred_element_type=jnp.float32).astype(jnp.bfloat16)


def normed(h):
    wide = h.astype(jnp.float32)
    scale = lax.rsqrt(jnp.mean(wide**2, -1, keepdims=True) + 1e-6)
    return (wide * scale).astype(jnp.bfloat16)


def turned(t, theta):
    half = t.shape[-1] // 2
    angle = jnp.arange(t.shape[0], dtype=jnp.float32)[:, None] * theta ** (-jnp.arange(half, dtype=jnp.float32) / half)
    cos, sin = jnp.cos(angle)[:, None], jnp.sin(angle)[:, None]
    a, b = t[..., :half].astype(jnp.float32), t[..., half:].astype(jnp.float32)
    return jnp.concatenate([a * cos - b * sin, b * cos + a * sin], -1).astype(jnp.bfloat16)


def seen_by(q, k, v):
    tokens, kv = q.shape[0], k.shape[1]
    q = q.reshape(tokens, kv, -1, q.shape[-1])
    scores = jnp.einsum("tgsd,ugd->gstu", q.astype(jnp.float32), k.astype(jnp.float32)) * q.shape[-1] ** -0.5
    place = jnp.arange(tokens)
    weights = jax.nn.softmax(jnp.where(place[:, None] >= place, scores, -jnp.inf), -1).astype(jnp.bfloat16)
    return jnp.einsum("gstu,ugd->tgsd", weights.astype(jnp.float32), v.astype(jnp.float32)).astype(jnp.bfloat16).reshape(tokens, -1)


def layer(h, w):
    a = normed(h)
    q, k = (turned(matmul(a, w[name]).reshape(h.shape[0], -1, HEAD), THETA) for name in ("wq", "wk"))
    h = h + matmul(seen_by(q, k, matmul(a, w["wv"]).reshape(h.shape[0], -1, HEAD)), w["wo"])
    b = normed(h)
    gate = jnp.dot(b, w["w_gate"], preferred_element_type=jnp.float32)
    up = jnp.dot(b, w["w_up"], preferred_element_type=jnp.float32)
    return h + matmul((jax.nn.silu(gate) * up).astype(jnp.bfloat16), w["w_down"])


def adamw(w, m, v, g):
    m = 0.9 * m + 0.1 * g
    v = 0.95 * v + 0.05 * g * g
    step = m * lax.rsqrt(v + 1e-8) + 0.1 * w
    return (w - 0.02 * step).astype(jnp.bfloat16), m, v


def stack(weights, h):
    return lax.scan(lambda h, w: (layer(h, w), None), h, weights)[0]


def reference(x, dy, wq, wk, wv, wo, w_gate, w_up, w_down, m_wq, m_wk, m_wv, m_wo, m_w_gate, m_w_up, m_w_down, v_wq, v_wk, v_wv, v_wo, v_w_gate, v_w_up, v_w_down):
    weights = dict(zip(NAMES, (wq, wk, wv, wo, w_gate, w_up, w_down), strict=True))

    def take(so_far, sequence):
        h, by_y = sequence
        _, back = jax.vjp(stack, weights, h)
        by_weights, by_h = back(by_y)
        return jax.tree.map(lambda total, term: total + term.astype(jnp.float32), so_far, by_weights), by_h

    none_yet = {name: jnp.zeros(w.shape, jnp.float32) for name, w in weights.items()}
    by_weights, by_x = lax.scan(take, none_yet, (x, dy))
    gradients = [by_weights[name].astype(jnp.bfloat16).astype(jnp.float32) for name in NAMES]
    first = (m_wq, m_wk, m_wv, m_wo, m_w_gate, m_w_up, m_w_down)
    second = (v_wq, v_wk, v_wv, v_wo, v_w_gate, v_w_up, v_w_down)
    new = [adamw(weights[name].astype(jnp.float32), m, v, g) for name, m, v, g in zip(NAMES, first, second, gradients, strict=True)]
    return tuple(one[which] for which in range(3) for one in new)
```

```python
import functools

import jax
import jax.numpy as jnp
import numpy as np
from jax import lax
from jax.experimental import pallas as pl
from jax.experimental.pallas import tpu as pltpu
from jax.sharding import PartitionSpec as P

NEG = -1e30
HIDDEN = 2 * NEG
LOG2E = 1.4426950408889634
VMEM = 56 * 2**20
STRIP = 512


def _dot(a, b, ca, cb):
    return lax.dot_general(a, b, (((ca,), (cb,)), ((), ())), preferred_element_type=jnp.float32)


def _seen(iq, bq, bk):
    return lax.div(iq * bq + 1, bk), lax.div(iq * bq + bq - 1 + bk, bk)


def _gap(bk, cols, bq):
    return lax.rem(lax.broadcasted_iota(jnp.int32, (bk, cols), 1), bq) - lax.broadcasted_iota(jnp.int32, (bk, cols), 0)


def _row(ref):
    return jnp.concatenate([ref[n : n + 1, :] for n in range(ref.shape[0])], axis=1)


def _attend_kernel(bq, bk, q_ref, k_ref, v_ref, o_ref, lse_ref, top_s, mix_s, gap_s):
    heads, _, d = q_ref.shape
    cols = heads * bq
    iq = pl.program_id(0)
    e = d**-0.5 * LOG2E
    pieces = range(0, cols, STRIP)

    @pl.when(iq == 0)
    def _():
        gap_s[...] = _gap(bk, cols, bq)

    top_s[...] = jnp.full(top_s.shape, NEG, jnp.float32)
    mix_s[...] = jnp.zeros(mix_s.shape, jnp.float32)
    ones = jnp.ones((8, bk), k_ref.dtype)

    def block(j, masked):
        here = pl.ds(j * bk, bk)
        q = q_ref[...].reshape(cols, d)
        scores = [_dot(k_ref[here, :], q[at : at + STRIP, :], 1, 1) for at in pieces]
        ok = gap_s[...] >= j * bk - iq * bq if masked else None
        weights, keeps = [], []
        for at, s in zip(pieces, scores):
            if masked:
                s = jnp.where(ok[:, at : at + STRIP], s, HIDDEN)
            old = top_s[:, at : at + STRIP]
            top = jnp.maximum(old, s.max(axis=0, keepdims=True))
            top_s[:, at : at + STRIP] = top
            weights.append(jnp.exp2((s - top) * e).astype(k_ref.dtype))
            keeps.append(jnp.exp2((old - top) * e))
        values = jnp.concatenate([v_ref[here, :].T, ones], axis=0)
        for at, p, keep in zip(pieces, weights, keeps):
            mix_s[:, at : at + STRIP] = mix_s[:, at : at + STRIP] * keep + _dot(values, p, 1, 0)

    whole, last = _seen(iq, bq, bk)
    lax.fori_loop(0, whole, lambda j, _: block(j, False), None)
    lax.fori_loop(whole, last, lambda j, _: block(j, True), None)
    total = mix_s[d : d + 1, :]
    o_ref[...] = (mix_s[:d, :] * (1 / total)).T.reshape(heads, bq, d).astype(o_ref.dtype)
    lse = top_s[...] * d**-0.5 + jnp.log(total)
    for n in range(heads):
        lse_ref[n : n + 1, :] = lse[:, n * bq : (n + 1) * bq]


def attend(q, k, v, bq=512, bk=512):
    heads, t, d = q.shape
    queries = pl.BlockSpec((heads, bq, d), lambda i: (0, i, 0))
    keys = pl.BlockSpec((t, d), lambda i: (0, 0))
    return pl.pallas_call(
        functools.partial(_attend_kernel, bq, bk),
        name="attend",
        grid=(t // bq,),
        in_specs=[queries, keys, keys],
        out_specs=[queries, pl.BlockSpec((heads, bq), lambda i: (0, i))],
        scratch_shapes=[pltpu.VMEM((1, heads * bq), jnp.float32), pltpu.VMEM((d + 8, heads * bq), jnp.float32),
                        pltpu.VMEM((bk, heads * bq), jnp.int32)],
        out_shape=[jax.ShapeDtypeStruct(q.shape, q.dtype), jax.ShapeDtypeStruct((heads, t), jnp.float32)],
        compiler_params=pltpu.CompilerParams(dimension_semantics=("arbitrary",), vmem_limit_bytes=VMEM),
        cost_estimate=pl.CostEstimate(flops=4 * q.size * t, bytes_accessed=4 * q.size, transcendentals=heads * t * t),
    )(q, k, v)


def _attend_bwd_kernel(bq, bk, q_ref, k_ref, v_ref, do_ref, lse_ref, delta_ref, dq_ref, dk_ref, dv_ref, dq_s, dk_s, dv_s, gap_s):
    heads, _, d = q_ref.shape
    low, cols = q_ref.dtype, heads * bq
    iq = pl.program_id(0)
    scale = d**-0.5
    pieces = range(0, cols, STRIP)

    @pl.when(iq == 0)
    def _():
        gap_s[...] = _gap(bk, cols, bq)
        dk_s[...] = jnp.zeros_like(dk_s)
        dv_s[...] = jnp.zeros_like(dv_s)

    dq_s[...] = jnp.zeros_like(dq_s)
    lses = _row(lse_ref) * LOG2E
    deltas = _row(delta_ref)

    def block(j, masked):
        here = pl.ds(j * bk, bk)
        qs = [q_ref[...].reshape(cols, d)[at : at + STRIP, :] for at in pieces]
        dos = [do_ref[...].reshape(cols, d)[at : at + STRIP, :] for at in pieces]
        scores = [_dot(k_ref[here, :], x, 1, 1) for x in qs]
        dps = [_dot(v_ref[here, :], x, 1, 1) for x in dos]
        ok = gap_s[...] >= j * bk - iq * bq if masked else None
        for n, at in enumerate(pieces):
            p = jnp.exp2(scores[n] * (scale * LOG2E) - lses[:, at : at + STRIP])
            if masked:
                p = jnp.where(ok[:, at : at + STRIP], p, 0.0)
            ds = (p * (dps[n] - deltas[:, at : at + STRIP])).astype(low)
            dv_s[here, :] += _dot(p.astype(low), dos[n], 1, 0)
            dk_s[here, :] += _dot(ds, qs[n], 1, 0)
            dq_s[:, at : at + STRIP] += _dot(k_ref[here, :].T, ds, 1, 0)

    whole, last = _seen(iq, bq, bk)
    lax.fori_loop(0, whole, lambda j, _: block(j, False), None)
    lax.fori_loop(whole, last, lambda j, _: block(j, True), None)
    dq_ref[...] = (dq_s[...] * scale).T.reshape(heads, bq, d).astype(dq_ref.dtype)

    @pl.when(iq == pl.num_programs(0) - 1)
    def _():
        dk_ref[...] = (dk_s[...] * scale).astype(dk_ref.dtype)
        dv_ref[...] = dv_s[...].astype(dv_ref.dtype)


def attend_bwd(q, k, v, d_out, lse, delta, bq=256, bk=512):
    heads, t, d = q.shape
    queries = pl.BlockSpec((heads, bq, d), lambda i: (0, i, 0))
    keys = pl.BlockSpec((t, d), lambda i: (0, 0))
    stats = pl.BlockSpec((heads, bq), lambda i: (0, i))
    return pl.pallas_call(
        functools.partial(_attend_bwd_kernel, bq, bk),
        name="attend_bwd",
        grid=(t // bq,),
        in_specs=[queries, keys, keys, queries, stats, stats],
        out_specs=[queries, keys, keys],
        scratch_shapes=[pltpu.VMEM((d, heads * bq), jnp.float32), pltpu.VMEM((t, d), jnp.float32), pltpu.VMEM((t, d), jnp.float32),
                        pltpu.VMEM((bk, heads * bq), jnp.int32)],
        out_shape=[jax.ShapeDtypeStruct(a.shape, a.dtype) for a in (q, k, v)],
        compiler_params=pltpu.CompilerParams(dimension_semantics=("arbitrary",), vmem_limit_bytes=VMEM),
        cost_estimate=pl.CostEstimate(flops=10 * q.size * t, bytes_accessed=8 * q.size, transcendentals=heads * t * t),
    )(q, k, v, d_out, lse, delta)


HEAD = 128
THETA = 10000
EPS = 1e-6
F32, BF16 = jnp.float32, jnp.bfloat16
ANY = pl.BlockSpec(memory_space=pl.ANY)


def _whole(shape):
    return pl.BlockSpec(shape, lambda *_: (0,) * len(shape), pipeline_mode=pl.Buffered(1))


def _layer(number, w):
    return pl.BlockSpec((None, *w.shape[1:]), lambda *_: (number, 0, 0), pipeline_mode=pl.Buffered(1))


def _rows(tm, cols):
    return pl.BlockSpec((tm, cols), lambda i: (i, 0))


def _columns(rows, tm):
    return pl.BlockSpec((rows, tm), lambda i: (0, i))


def _heads(n, tm):
    return pl.BlockSpec((n, tm, HEAD), lambda i: (0, i, 0))


def _call(kernel, name, grid, in_specs, out_specs, out_shape, flops, scratch=(), order="arbitrary"):
    moved = sum(s.size * s.dtype.itemsize for s in out_shape)
    return pl.pallas_call(
        kernel,
        name=name,
        grid=grid,
        in_specs=in_specs,
        out_specs=out_specs,
        out_shape=out_shape,
        scratch_shapes=list(scratch),
        compiler_params=pltpu.CompilerParams(dimension_semantics=(order,) * len(grid), vmem_limit_bytes=VMEM),
        cost_estimate=pl.CostEstimate(flops=flops, bytes_accessed=2 * moved, transcendentals=0),
    )


def _like(*shape, dtype=BF16):
    return jax.ShapeDtypeStruct(shape, dtype)


def _normed(h):
    wide = h.astype(F32)
    scale = lax.rsqrt(jnp.mean(wide * wide, -1, keepdims=True) + EPS)
    return (wide * scale).astype(BF16), wide, scale


def _normed_bwd(d, wide, scale):
    return scale * (d - wide * (scale * scale * jnp.mean(d * wide, -1, keepdims=True)))


def _sigmoid(x):
    return 0.5 * jnp.tanh(0.5 * x) + 0.5


def _turn(t, cos, sin):
    return t * cos + pltpu.roll(t, HEAD // 2, 1) * sin


def _tables(tokens):
    half = HEAD // 2
    angle = np.arange(tokens, dtype=np.float32)[:, None] * (np.float32(THETA) ** (-np.arange(half, dtype=np.float32) / np.float32(half)))
    angle = angle.astype(np.float64)
    cos, sin = np.cos(angle).astype(np.float32), np.sin(angle).astype(np.float32)
    return jnp.asarray(np.concatenate([cos, cos], 1)), jnp.asarray(np.concatenate([-sin, sin], 1))


def _qkv_kernel(heads, h_ref, wq_ref, wk_ref, wv_ref, cos_ref, sin_ref, at_ref, q_ref, k_ref, v_ref):
    a, _, _ = _normed(h_ref[...])
    at_ref[...] = a.T
    cos, sin = cos_ref[...], sin_ref[...]
    q = _dot(a, wq_ref[...], 1, 0).astype(BF16).astype(F32)
    for n in range(heads):
        q_ref[n] = _turn(q[:, n * HEAD : (n + 1) * HEAD], cos, sin).astype(BF16)
    k_ref[...] = _turn(_dot(a, wk_ref[...], 1, 0).astype(BF16).astype(F32), cos, sin).astype(BF16)
    v_ref[...] = _dot(a, wv_ref[...], 1, 0).astype(BF16)


def qkv(number, h, wq, wk, wv, cos, sin, tm=512):
    t, d = h.shape
    heads = wq.shape[2] // HEAD
    return _call(
        functools.partial(_qkv_kernel, heads), "qkv", (t // tm,),
        [_rows(tm, d), *(_layer(number, w) for w in (wq, wk, wv)), _rows(tm, HEAD), _rows(tm, HEAD)],
        [_columns(d, tm), _heads(heads, tm), _rows(tm, HEAD), _rows(tm, HEAD)],
        [_like(d, t), _like(heads, t, HEAD), _like(t, HEAD), _like(t, HEAD)],
        2 * t * d * (heads + 2) * HEAD,
    )(h, wq, wk, wv, cos, sin)


def _first_half(o_ref, h_ref, wo_ref, ot_ref):
    o = jnp.concatenate([o_ref[n] for n in range(o_ref.shape[0])], axis=1)
    ot_ref[...] = o.T
    h1 = h_ref[...].astype(F32) + _dot(o, wo_ref[...], 1, 0).astype(BF16).astype(F32)
    return h1.astype(BF16)


def _forward_mlp(chunk, o_ref, h_ref, wo_ref, wg_ref, wu_ref, wd_ref, ot_ref, h1_ref, bt_ref, gu_ref, actt_ref, *h2_ref):
    h1 = _first_half(o_ref, h_ref, wo_ref, ot_ref)
    h1_ref[...] = h1
    b, _, _ = _normed(h1)
    bt_ref[...] = b.T
    ff = wg_ref.shape[1]
    y = jnp.zeros(h1.shape, F32)
    for at in range(0, ff, chunk):
        gate = _dot(b, wg_ref[:, at : at + chunk], 1, 0)
        up = _dot(b, wu_ref[:, at : at + chunk], 1, 0)
        gu_ref[:, at : at + chunk] = gate
        gu_ref[:, ff + at : ff + at + chunk] = up
        act = (gate * _sigmoid(gate) * up).astype(BF16)
        actt_ref[at : at + chunk, :] = act.T
        if h2_ref:
            y += _dot(act, wd_ref[at : at + chunk, :], 1, 0)
    if h2_ref:
        h2_ref[0][...] = (h1.astype(F32) + y.astype(BF16).astype(F32)).astype(BF16)


def forward_mlp(number, o, h, wo, wg, wu, wd, last, tm=256, chunk=640):
    (heads, t, _), d, ff = o.shape, h.shape[1], wg.shape[2]
    return _call(
        functools.partial(_forward_mlp, chunk), "forward_mlp", (t // tm,),
        [_heads(heads, tm), _rows(tm, d), *(_layer(number, w) for w in (wo, wg, wu, wd))],
        [_columns(heads * HEAD, tm), _rows(tm, d), _columns(d, tm), _rows(tm, 2 * ff), _columns(ff, tm), _rows(tm, d)][: 5 if last else 6],
        [_like(heads * HEAD, t), _like(t, d), _like(d, t), _like(t, 2 * ff, dtype=F32), _like(ff, t), _like(t, d)][: 5 if last else 6],
        2 * t * d * (heads * HEAD + (2 if last else 3) * ff),
    )(o, h, wo, wg, wu, wd)


def _back(chunk, dy, h1, gate_up, o_ref, wo_ref, wg_ref, wu_ref, wd_ref, dgu_ref, dh1_ref, do_ref, delta_ref):
    ff = wg_ref.shape[1]
    db = jnp.zeros(dy.shape, F32)
    for at in range(0, ff, chunk):
        gate, up = gate_up(at)
        by = _dot(dy, wd_ref[at : at + chunk, :], 1, 1).astype(BF16).astype(F32)
        s = _sigmoid(gate)
        silu = gate * s
        dup = (by * silu).astype(BF16)
        dgate = (by * up * (s + silu * (1 - s))).astype(BF16)
        dgu_ref[:, at : at + chunk] = dgate
        dgu_ref[:, ff + at : ff + at + chunk] = dup
        db += _dot(dgate, wg_ref[:, at : at + chunk], 1, 1) + _dot(dup, wu_ref[:, at : at + chunk], 1, 1)
    _, wide, scale = _normed(h1)
    dn = _normed_bwd(db.astype(BF16).astype(F32), wide, scale).astype(BF16)
    dh1 = (dy.astype(F32) + dn.astype(F32)).astype(BF16)
    dh1_ref[...] = dh1
    do = _dot(dh1, wo_ref[...], 1, 1).astype(BF16)
    for n in range(o_ref.shape[0]):
        mine = do[:, n * HEAD : (n + 1) * HEAD]
        do_ref[n] = mine
        delta_ref[n : n + 1, :] = (mine.astype(F32) * o_ref[n].astype(F32)).T.sum(0, keepdims=True)


def _backward_mlp(chunk, dy_ref, h1_ref, gu_ref, o_ref, wo_ref, wg_ref, wu_ref, wd_ref, dgu_ref, dh1_ref, do_ref, delta_ref):
    ff = wg_ref.shape[1]
    kept = lambda at: (gu_ref[:, at : at + chunk], gu_ref[:, ff + at : ff + at + chunk])
    _back(chunk, dy_ref[...], h1_ref[...], kept, o_ref, wo_ref, wg_ref, wu_ref, wd_ref, dgu_ref, dh1_ref, do_ref, delta_ref)


def backward_mlp(number, dy, h1, gu, o, wo, wg, wu, wd, tm=256, chunk=640):
    (heads, t, _), d, ff = o.shape, h1.shape[1], wg.shape[2]
    return _call(
        functools.partial(_backward_mlp, chunk), "backward_mlp", (t // tm,),
        [_rows(tm, d), _rows(tm, d), _rows(tm, 2 * ff), _heads(heads, tm), *(_layer(number, w) for w in (wo, wg, wu, wd))],
        [_rows(tm, 2 * ff), _rows(tm, d), _heads(heads, tm), _columns(heads, tm)],
        [_like(t, 2 * ff), _like(t, d), _like(heads, t, HEAD), _like(heads, t, dtype=F32)],
        2 * t * d * (heads * HEAD + 3 * ff),
    )(dy, h1, gu, o, wo, wg, wu, wd)


def _qkv_bwd_kernel(dq_ref, dk_ref, dv_ref, cos_ref, sin_ref, *rest):
    cos, sin = cos_ref[...], -sin_ref[...]
    parts = [_turn(dq_ref[n].astype(F32), cos, sin).astype(BF16) for n in range(dq_ref.shape[0])]
    parts += [_turn(dk_ref[...].astype(F32), cos, sin).astype(BF16), dv_ref[...]]
    dqkv_ref = rest[-1] if len(rest) == 1 else rest[-2]
    for n, part in enumerate(parts):
        dqkv_ref[:, n * HEAD : (n + 1) * HEAD] = part
    if len(rest) > 1:
        h_ref, dh1_ref, wq_ref, wk_ref, wv_ref, _, dh_ref = rest
        da = _dot(jnp.concatenate(parts[:-2], 1), wq_ref[...], 1, 1) + _dot(parts[-2], wk_ref[...], 1, 1) + _dot(parts[-1], wv_ref[...], 1, 1)
        _, wide, scale = _normed(h_ref[...])
        dn = _normed_bwd(da.astype(BF16).astype(F32), wide, scale).astype(BF16)
        dh_ref[...] = (dh1_ref[...].astype(F32) + dn.astype(F32)).astype(BF16)


def qkv_bwd(number, dq, dk, dv, cos, sin, more=None, tm=512):
    heads, t, _ = dq.shape
    width = (heads + 2) * HEAD
    ins, outs, shapes, d = [_heads(heads, tm)] + [_rows(tm, HEAD)] * 4, [_rows(tm, width)], [_like(t, width)], 1
    if more is not None:
        d = more[0].shape[1]
        ins += [_rows(tm, d), _rows(tm, d), *(_layer(number, w) for w in more[2:])]
        outs, shapes = outs + [_rows(tm, d)], shapes + [_like(t, d)]
    return _call(_qkv_bwd_kernel, "qkv_bwd", (t // tm,), ins, outs, shapes, 2 * t * d * width)(dq, dk, dv, cos, sin, *(more or ()))


def _weight_rows(left_ref, right_ref, *rest):
    out_ref = rest[-1]
    out_ref[...] = _dot(left_ref[...], right_ref[...], 1, 0).astype(BF16).reshape(out_ref.shape)


def _weight_columns(tn, left_ref, right_ref, out_ref):
    devices, r = out_ref.shape[0], left_ref.shape[0] // out_ref.shape[0]
    g = _dot(left_ref[...], right_ref[...], 1, 0).astype(BF16)
    for n in range(g.shape[1] // tn):
        out_ref[:, n * r : (n + 1) * r, :] = g[:, n * tn : (n + 1) * tn].reshape(devices, r, tn)


def weight_columns(left, right, devices, rows_all, tn, wide=640):
    (rows, t), n = left.shape, right.shape[1]
    r = rows // devices
    return pl.pallas_call(
        functools.partial(_weight_columns, tn),
        name="weight_columns",
        grid=(n // wide,),
        in_specs=[_whole((rows, t)), pl.BlockSpec((t, wide), lambda j: (0, j))],
        out_specs=pl.BlockSpec((devices, r * (wide // tn), tn), lambda j: (0, j, 0)),
        out_shape=_like(devices, rows_all, tn),
        compiler_params=pltpu.CompilerParams(dimension_semantics=("arbitrary",), vmem_limit_bytes=VMEM),
        cost_estimate=pl.CostEstimate(flops=2 * rows * t * n, bytes_accessed=2 * (rows * t + t * n + rows * n), transcendentals=0),
    )(left, right)


def weight_rows(left, right, devices, per, into=None, at=0):
    (rows, t), n = left.shape, right.shape[1]
    r = rows // devices
    given, specs, alias = [left, right], [pl.BlockSpec((per * r, t), lambda i: (i, 0)), _whole((t, n))], {}
    if into is not None:
        given, specs, alias = given + [into], specs + [ANY], {2: 0}
    return pl.pallas_call(
        _weight_rows,
        name="weight_rows",
        grid=(devices // per,),
        in_specs=specs,
        out_specs=pl.BlockSpec((pl.Element(per), pl.Element(r), pl.Element(n)), lambda i: (i * per, at, 0)) if at else pl.BlockSpec((per, r, n), lambda i: (i, 0, 0)),
        out_shape=_like(devices, r, n) if into is None else _like(*into.shape),
        input_output_aliases=alias,
        compiler_params=pltpu.CompilerParams(dimension_semantics=("arbitrary",), vmem_limit_bytes=VMEM),
        cost_estimate=pl.CostEstimate(flops=2 * rows * t * n, bytes_accessed=2 * (rows * t + t * n + rows * n), transcendentals=0),
    )(*given)


def adamw(w, m, v, g):
    m = 0.9 * m + 0.1 * g
    v = 0.95 * v + 0.05 * g * g
    step = m * lax.rsqrt(v + 1e-8) + 0.1 * w
    return (w - 0.02 * step).astype(BF16), m, v


def _adamw_kernel(rows, tn, terms, me_ref, *rest):
    k = len(rows)
    g_refs, rest = rest[:terms], rest[terms:]
    w_refs, m_refs, v_refs = (rest[i * k : (i + 1) * k] for i in range(3))
    new_ref, *outs = rest[-1 - 2 * k :]
    at = 0
    for i, r in enumerate(rows):
        for left in range(0, w_refs[i].shape[2], tn):
            here = (0, slice(None), slice(left, left + tn))
            g = g_refs[0][at : at + r, :].astype(F32)
            for ref in g_refs[1:]:
                g += ref[at : at + r, :].astype(F32)
            g = g.astype(BF16).astype(F32)
            new, m, v = adamw(w_refs[i][here].astype(F32), m_refs[i][here], v_refs[i][here], g)
            new_ref[at : at + r, :], outs[i][here], outs[k + i][here] = new, m, v
            at += r


def adamw_step(me, number, g, ws, ms, vs, before):
    terms, g = g, g[0]
    tn = g.shape[1]
    layers, rows = ms[0].shape[0], [m.shape[1] for m in ms]
    mine = lambda m: pl.BlockSpec((1, *m.shape[1:]), lambda i, me: (number, me[0], 0))
    moment = lambda m: pl.BlockSpec((1, *m.shape[1:]), lambda i, me: (number, 0, 0))
    flat = pl.BlockSpec(g.shape, lambda i, me: (0, 0))
    given = [*terms, *ws, *ms, *vs]
    specs = [*[flat] * len(terms), *map(mine, ms), *map(moment, ms), *map(moment, vs)]
    alias = {}
    if before is not None:
        alias = {1 + len(given) + i: 1 + i for i in range(len(before))}
        given += before
        specs += [ANY] * len(before)
    new, *moments = pl.pallas_call(
        functools.partial(_adamw_kernel, rows, tn, len(terms)),
        name="adamw",
        grid_spec=pltpu.PrefetchScalarGridSpec(
            num_scalar_prefetch=1, grid=(1,), in_specs=specs, out_specs=[flat, *map(moment, ms), *map(moment, vs)],
        ),
        out_shape=[_like(*g.shape)] + [_like(*m.shape, dtype=F32) for m in (*ms, *vs)],
        input_output_aliases=alias,
        compiler_params=pltpu.CompilerParams(dimension_semantics=("arbitrary",), vmem_limit_bytes=VMEM),
        cost_estimate=pl.CostEstimate(flops=20 * g.size, bytes_accessed=30 * g.size, transcendentals=g.size),
    )(me, *given)
    return new, moments


def _spread_kernel(numbers, rows, *refs):
    k = len(rows)
    all_ref, outs = refs[0], refs[-3 - k : -3]
    here, in_sem, out_sem = refs[-3:]
    devices = all_ref.shape[0]
    tn = all_ref.shape[2]
    ins = [pltpu.make_async_copy(all_ref.at[j], here.at[j], in_sem.at[j]) for j in range(devices)]
    for copy in ins:
        copy.start()
    out = []
    for j, copy in enumerate(ins):
        copy.wait()
        at = n = 0
        for number, ref, r in [(number, *one) for number in numbers for one in zip(outs, rows)]:
            for left in range(0, ref.shape[2], tn):
                target = ref.at[number, pl.ds(j * r, r), pl.ds(left, tn)]
                out.append(pltpu.make_async_copy(here.at[j, pl.ds(at, r), :], target, out_sem.at[j, n]))
                out[-1].start()
                at, n = at + r, n + 1
    for copy in out:
        copy.wait()


def spread(numbers, everyone, shapes, before):
    devices, total, tn = everyone.shape
    rows = [s[1] // devices for s in shapes]
    tiles = len(numbers) * sum(s[2] // tn for s in shapes)
    given, alias = [everyone], {}
    if before is not None:
        alias = {1 + i: i for i in range(len(before))}
        given += before
    return pl.pallas_call(
        functools.partial(_spread_kernel, numbers, rows),
        name="spread",
        in_specs=[ANY] * len(given),
        out_specs=[ANY] * len(shapes),
        out_shape=[_like(*s) for s in shapes],
        scratch_shapes=[pltpu.VMEM(everyone.shape, BF16), pltpu.SemaphoreType.DMA((devices,)), pltpu.SemaphoreType.DMA((devices, tiles))],
        input_output_aliases=alias,
        compiler_params=pltpu.CompilerParams(vmem_limit_bytes=VMEM),
        cost_estimate=pl.CostEstimate(flops=everyone.size, bytes_accessed=4 * everyone.size, transcendentals=0),
    )(*given)


def solution(mesh):
    devices = mesh.shape["dp"]
    chips = devices // 2
    rightward = [(i, (i + 2) % devices) for i in range(devices)]
    leftward = [(i, (i - 2) % devices) for i in range(devices)]
    across = [(i, i ^ 1) for i in range(devices)]
    send = lambda a, way: lax.ppermute(a, "dp", way)

    def ringed(terms):
        chip, core = lax.axis_index("dp") // 2, lax.axis_index("dp") % 2
        _, r, n = terms.shape
        terms = terms.reshape(chips, 2, r, n)
        keep = lax.dynamic_index_in_dim(terms, core, 1, False)
        got = send(lax.dynamic_index_in_dim(terms, 1 - core, 1, False), across)
        block = lambda step: [lax.dynamic_index_in_dim(a, (chip + step) % chips, 0, False) for a in (keep, got)]
        both = lambda step: sum(a.astype(F32) for a in block(step))
        cut = r // 2
        far = both(2)
        first, second = send(far[:cut].astype(BF16), rightward), send(far[cut:].astype(BF16), leftward)
        nexts, prevs = both(1), both(-1)
        nexts = jnp.concatenate([nexts[:cut] + first.astype(F32), nexts[cut:]], 0)
        prevs = jnp.concatenate([prevs[:cut], prevs[cut:] + second.astype(F32)], 0)
        return [*block(0), send(nexts.astype(BF16), rightward), send(prevs.astype(BF16), leftward)]

    def step(x, dy, *arrays):
        weights, m, v = (arrays[i : i + 7] for i in (0, 7, 14))
        wq, wk, wv, wo, wg, wu, wd = weights
        layers = wq.shape[0]
        me = jnp.reshape(lax.axis_index("dp"), (1,))
        cos, sin = _tables(x.shape[1])
        groups = {"d": (6,), "guo": (4, 5, 3), "qkv": (0, 1, 2)}
        moments = {name: None for name in groups}
        whole = {name: None for name in groups}

        summed = lambda terms: [lax.psum_scatter(terms, "dp", scatter_dimension=0, tiled=False)]
        gathered = lambda new: lax.all_gather(new, "dp", axis=0, tiled=False)
        after = lax.optimization_barrier

        def stepped(name, number, g):
            which = groups[name]
            new, moments[name] = adamw_step(me, number, g, *([s[i] for i in which] for s in (weights, m, v)), moments[name])
            return new

        def place(name, everyone, *numbers):
            whole[name] = spread(numbers, everyone, [weights[i].shape for i in groups[name]], whole[name])

        h, kept = x[0], []
        for i in range(layers):
            at, q, k, val = qkv(i, h, wq, wk, wv, cos, sin)
            o, lse = attend(q, k, val)
            ot, h1, bt, gu, actt, *result = forward_mlp(i, o, h, wo, wg, wu, wd, i == layers - 1)
            kept.append((h, at, q, k, val, o, lse, ot, h1, bt, gu, actt))
            h = result[0] if result else None
        dh = dy[0]
        behind, fresh_qkv = [], []
        for i in reversed(range(layers)):
            h, at, q, k, val, o, lse, ot, h1, bt, gu, actt = kept[i]
            by_d = weight_rows(actt, dh, devices, 1)
            gu, by_d = after((gu, by_d))
            g_d = summed(by_d)
            dgu, dh1, do, delta = backward_mlp(i, dh, h1, gu, o, wo, wg, wu, wd)
            first_one = not behind
            if first_one:
                dgu, g_d = after((dgu, g_d))
                new_d = stepped("d", i, g_d)
                dgu, new_d = after((dgu, new_d))
                all_d = gathered(new_d)
            else:
                dgu, all_guo = after((dgu, behind[0]))
                place("guo", all_guo, i + 1)
            r = sum(wo.shape[1:2] + (wg.shape[1] * wg.shape[2] // 320,)) // devices
            by_guo = weight_columns(bt, dgu, devices, r, 640)
            by_guo = weight_rows(ot, dh1, devices, devices // 2, by_guo, r - wo.shape[1] // devices)
            if first_one:
                do, by_guo, all_d = after((do, by_guo, all_d))
            else:
                do, by_guo, g_d, g_qkv = after((do, by_guo, g_d, behind[1]))
                new_d = stepped("d", i, g_d)
                fresh_qkv.append(stepped("qkv", i + 1, g_qkv))
                do, by_guo, new_d, fresh_qkv = after((do, by_guo, new_d, fresh_qkv))
            g_guo = summed(by_guo)
            dq, dk, dv = attend_bwd(q, k, val, do, lse, delta)
            dq, g_guo = after((dq, g_guo))
            new_guo = stepped("guo", i, g_guo)
            dq, new_guo = after((dq, new_guo))
            if not first_one:
                all_d = gathered(new_d)
            all_guo = gathered(new_guo)
            got = qkv_bwd(i, dq, dk, dv, cos, sin, (h, dh1, wq, wk, wv) if i else None)
            by_qkv = weight_columns(at, got[0], devices, got[0].shape[1] // HEAD * at.shape[0] // devices, HEAD)
            if i:
                dh, by_qkv = after((got[-1], by_qkv))
            elif not first_one:
                by_qkv, all_d = after((by_qkv, all_d))
            place("d", all_d, i)
            behind = [all_guo, summed(by_qkv) if i else ringed(by_qkv)]
        fresh_qkv.append(stepped("qkv", 0, behind[1]))
        all_guo, fresh_qkv = after((behind[0], fresh_qkv))
        place("guo", all_guo, 0)
        place("qkv", gathered(jnp.concatenate(fresh_qkv, 0)), *reversed(range(layers)))
        new, first, second = [None] * 7, [None] * 7, [None] * 7
        for name, which in groups.items():
            for n, i in enumerate(which):
                new[i], first[i], second[i] = whole[name][n], moments[name][n], moments[name][len(which) + n]
        return (*new, *first, *second)

    states, all_of, cut = P(("rep", "dp"), None, None), P(None, None, None), P(None, "dp", None)
    return jax.shard_map(
        step,
        mesh=mesh,
        in_specs=(states, states) + (all_of,) * 7 + (cut,) * 14,
        out_specs=(P("rep", None, None),) * 7 + (P("rep", "dp", None),) * 14,
        check_vma=False,
    )
```

```python
import functools

import jax
import jax.numpy as jnp
import numpy as np
from jax import lax
from jax.experimental import pallas as pl
from jax.experimental.pallas import tpu as pltpu
from jax.sharding import PartitionSpec as P

NEG = -1e30
HIDDEN = 2 * NEG
LOG2E = 1.4426950408889634
VMEM = 56 * 2**20
STRIP = 512
STRIP_BWD = 1024


def _dot(a, b, ca, cb):
    return lax.dot_general(a, b, (((ca,), (cb,)), ((), ())), preferred_element_type=jnp.float32)


def _seen(iq, bq, bk):
    return lax.div(iq * bq + 1, bk), lax.div(iq * bq + bq - 1 + bk, bk)


def _gap(bk, cols, bq):
    return lax.rem(lax.broadcasted_iota(jnp.int32, (bk, cols), 1), bq) - lax.broadcasted_iota(jnp.int32, (bk, cols), 0)


def _row(ref):
    return jnp.concatenate([ref[n : n + 1, :] for n in range(ref.shape[0])], axis=1)


def _attend_kernel(bq, bk, q_ref, k_ref, v_ref, o_ref, lse_ref, top_s, mix_s, gap_s):
    heads, _, d = q_ref.shape
    cols = heads * bq
    iq = pl.program_id(0)
    e = d**-0.5 * LOG2E
    pieces = range(0, cols, STRIP)

    @pl.when(iq == 0)
    def _():
        gap_s[...] = _gap(bk, cols, bq)

    top_s[...] = jnp.full(top_s.shape, NEG, jnp.float32)
    mix_s[...] = jnp.zeros(mix_s.shape, jnp.float32)
    ones = jnp.ones((8, bk), k_ref.dtype)

    def block(j, masked):
        here = pl.ds(j * bk, bk)
        q = q_ref[...].reshape(cols, d)
        scores = [_dot(k_ref[here, :], q[at : at + STRIP, :], 1, 1) for at in pieces]
        ok = gap_s[...] >= j * bk - iq * bq if masked else None
        weights, keeps = [], []
        for at, s in zip(pieces, scores):
            if masked:
                s = jnp.where(ok[:, at : at + STRIP], s, HIDDEN)
            old = top_s[:, at : at + STRIP]
            top = jnp.maximum(old, s.max(axis=0, keepdims=True))
            top_s[:, at : at + STRIP] = top
            weights.append(jnp.exp2((s - top) * e).astype(k_ref.dtype))
            keeps.append(jnp.exp2((old - top) * e))
        values = jnp.concatenate([v_ref[here, :].T, ones], axis=0)
        for at, p, keep in zip(pieces, weights, keeps):
            mix_s[:, at : at + STRIP] = mix_s[:, at : at + STRIP] * keep + _dot(values, p, 1, 0)

    whole, last = _seen(iq, bq, bk)
    lax.fori_loop(0, whole, lambda j, _: block(j, False), None)
    lax.fori_loop(whole, last, lambda j, _: block(j, True), None)
    total = mix_s[d : d + 1, :]
    o_ref[...] = (mix_s[:d, :] * (1 / total)).T.reshape(heads, bq, d).astype(o_ref.dtype)
    lse = top_s[...] * d**-0.5 + jnp.log(total)
    for n in range(heads):
        lse_ref[n : n + 1, :] = lse[:, n * bq : (n + 1) * bq]


def attend(q, k, v, bq=512, bk=512):
    heads, t, d = q.shape
    queries = pl.BlockSpec((heads, bq, d), lambda i: (0, i, 0))
    keys = pl.BlockSpec((t, d), lambda i: (0, 0))
    return pl.pallas_call(
        functools.partial(_attend_kernel, bq, bk),
        name="attend",
        grid=(t // bq,),
        in_specs=[queries, keys, keys],
        out_specs=[queries, pl.BlockSpec((heads, bq), lambda i: (0, i))],
        scratch_shapes=[pltpu.VMEM((1, heads * bq), jnp.float32), pltpu.VMEM((d + 8, heads * bq), jnp.float32),
                        pltpu.VMEM((bk, heads * bq), jnp.int32)],
        out_shape=[jax.ShapeDtypeStruct(q.shape, q.dtype), jax.ShapeDtypeStruct((heads, t), jnp.float32)],
        compiler_params=pltpu.CompilerParams(dimension_semantics=("arbitrary",), vmem_limit_bytes=VMEM),
        cost_estimate=pl.CostEstimate(flops=4 * q.size * t, bytes_accessed=4 * q.size, transcendentals=heads * t * t),
    )(q, k, v)


def _attend_bwd_kernel(bq, bk, q_ref, k_ref, v_ref, do_ref, lse_ref, delta_ref, dq_ref, dk_ref, dv_ref, dq_s, dk_s, dv_s, gap_s):
    heads, _, d = q_ref.shape
    low, cols = q_ref.dtype, heads * bq
    iq = pl.program_id(0)
    scale = d**-0.5
    pieces = range(0, cols, STRIP_BWD)

    @pl.when(iq == 0)
    def _():
        gap_s[...] = _gap(bk, cols, bq)
        dk_s[...] = jnp.zeros_like(dk_s)
        dv_s[...] = jnp.zeros_like(dv_s)

    dq_s[...] = jnp.zeros_like(dq_s)
    lses = _row(lse_ref) * LOG2E
    deltas = _row(delta_ref)

    def block(j, masked):
        here = pl.ds(j * bk, bk)
        qs = [q_ref[...].reshape(cols, d)[at : at + STRIP_BWD, :] for at in pieces]
        dos = [do_ref[...].reshape(cols, d)[at : at + STRIP_BWD, :] for at in pieces]
        scores = [_dot(k_ref[here, :], x, 1, 1) for x in qs]
        dps = [_dot(v_ref[here, :], x, 1, 1) for x in dos]
        ok = gap_s[...] >= j * bk - iq * bq if masked else None
        for n, at in enumerate(pieces):
            p = jnp.exp2(scores[n] * (scale * LOG2E) - lses[:, at : at + STRIP_BWD])
            if masked:
                p = jnp.where(ok[:, at : at + STRIP_BWD], p, 0.0)
            ds = (p * (dps[n] - deltas[:, at : at + STRIP_BWD])).astype(low)
            dv_s[here, :] += _dot(p.astype(low), dos[n], 1, 0)
            dk_s[here, :] += _dot(ds, qs[n], 1, 0)
            dq_s[:, at : at + STRIP_BWD] += _dot(k_ref[here, :].T, ds, 1, 0)

    whole, last = _seen(iq, bq, bk)
    lax.fori_loop(0, whole, lambda j, _: block(j, False), None)
    lax.fori_loop(whole, last, lambda j, _: block(j, True), None)
    dq_ref[...] = (dq_s[...] * scale).T.reshape(heads, bq, d).astype(dq_ref.dtype)

    @pl.when(iq == pl.num_programs(0) - 1)
    def _():
        dk_ref[...] = (dk_s[...] * scale).astype(dk_ref.dtype)
        dv_ref[...] = dv_s[...].astype(dv_ref.dtype)


def attend_bwd(q, k, v, d_out, lse, delta, bq=256, bk=256):
    heads, t, d = q.shape
    queries = pl.BlockSpec((heads, bq, d), lambda i: (0, i, 0))
    keys = pl.BlockSpec((t, d), lambda i: (0, 0))
    stats = pl.BlockSpec((heads, bq), lambda i: (0, i))
    return pl.pallas_call(
        functools.partial(_attend_bwd_kernel, bq, bk),
        name="attend_bwd",
        grid=(t // bq,),
        in_specs=[queries, keys, keys, queries, stats, stats],
        out_specs=[queries, keys, keys],
        scratch_shapes=[pltpu.VMEM((d, heads * bq), jnp.float32), pltpu.VMEM((t, d), jnp.float32), pltpu.VMEM((t, d), jnp.float32),
                        pltpu.VMEM((bk, heads * bq), jnp.int32)],
        out_shape=[jax.ShapeDtypeStruct(a.shape, a.dtype) for a in (q, k, v)],
        compiler_params=pltpu.CompilerParams(dimension_semantics=("arbitrary",), vmem_limit_bytes=VMEM),
        cost_estimate=pl.CostEstimate(flops=10 * q.size * t, bytes_accessed=8 * q.size, transcendentals=heads * t * t),
    )(q, k, v, d_out, lse, delta)


HEAD = 128
THETA = 10000
EPS = 1e-6
F32, BF16 = jnp.float32, jnp.bfloat16
ANY = pl.BlockSpec(memory_space=pl.ANY)


def _whole(shape):
    return pl.BlockSpec(shape, lambda *_: (0,) * len(shape), pipeline_mode=pl.Buffered(1))


def _layer(number, w):
    return pl.BlockSpec((None, *w.shape[1:]), lambda *_: (number, 0, 0), pipeline_mode=pl.Buffered(1))


def _rows(tm, cols):
    return pl.BlockSpec((tm, cols), lambda i: (i, 0))


def _columns(rows, tm):
    return pl.BlockSpec((rows, tm), lambda i: (0, i))


def _heads(n, tm):
    return pl.BlockSpec((n, tm, HEAD), lambda i: (0, i, 0))


def _call(kernel, name, grid, in_specs, out_specs, out_shape, flops, scratch=(), order="arbitrary"):
    moved = sum(s.size * s.dtype.itemsize for s in out_shape)
    return pl.pallas_call(
        kernel,
        name=name,
        grid=grid,
        in_specs=in_specs,
        out_specs=out_specs,
        out_shape=out_shape,
        scratch_shapes=list(scratch),
        compiler_params=pltpu.CompilerParams(dimension_semantics=(order,) * len(grid), vmem_limit_bytes=VMEM),
        cost_estimate=pl.CostEstimate(flops=flops, bytes_accessed=2 * moved, transcendentals=0),
    )


def _like(*shape, dtype=BF16):
    return jax.ShapeDtypeStruct(shape, dtype)


def _normed(h):
    wide = h.astype(F32)
    scale = lax.rsqrt(jnp.mean(wide * wide, -1, keepdims=True) + EPS)
    return (wide * scale).astype(BF16), wide, scale


def _normed_bwd(d, wide, scale):
    return scale * (d - wide * (scale * scale * jnp.mean(d * wide, -1, keepdims=True)))


def _chunks(ff):
    ends = [*range(768, ff - 768, 768), ff]
    return list(zip([0, *ends], ends))


def _sigmoid(x):
    return 0.5 * jnp.tanh(0.5 * x) + 0.5


def _turn(t, cos, sin):
    return t * cos + pltpu.roll(t, HEAD // 2, 1) * sin


def _tables(tokens):
    half = HEAD // 2
    angle = np.arange(tokens, dtype=np.float32)[:, None] * (np.float32(THETA) ** (-np.arange(half, dtype=np.float32) / np.float32(half)))
    angle = angle.astype(np.float64)
    cos, sin = np.cos(angle).astype(np.float32), np.sin(angle).astype(np.float32)
    return jnp.asarray(np.concatenate([cos, cos], 1)), jnp.asarray(np.concatenate([-sin, sin], 1))


def _qkv_kernel(heads, h_ref, wq_ref, wk_ref, wv_ref, cos_ref, sin_ref, at_ref, q_ref, k_ref, v_ref):
    a, _, _ = _normed(h_ref[...])
    at_ref[...] = a.T
    cos, sin = cos_ref[...], sin_ref[...]
    q = _dot(a, wq_ref[...], 1, 0).astype(BF16).astype(F32)
    for n in range(heads):
        q_ref[n] = _turn(q[:, n * HEAD : (n + 1) * HEAD], cos, sin).astype(BF16)
    kv = _dot(a, jnp.concatenate([wk_ref[...], wv_ref[...]], 1), 1, 0).astype(BF16)
    k_ref[...] = _turn(kv[:, :HEAD].astype(F32), cos, sin).astype(BF16)
    v_ref[...] = kv[:, HEAD:]


def qkv(number, h, wq, wk, wv, cos, sin, tm=512):
    t, d = h.shape
    heads = wq.shape[2] // HEAD
    return _call(
        functools.partial(_qkv_kernel, heads), "qkv", (t // tm,),
        [_rows(tm, d), *(_layer(number, w) for w in (wq, wk, wv)), _rows(tm, HEAD), _rows(tm, HEAD)],
        [_columns(d, tm), _heads(heads, tm), _rows(tm, HEAD), _rows(tm, HEAD)],
        [_like(d, t), _like(heads, t, HEAD), _like(t, HEAD), _like(t, HEAD)],
        2 * t * d * (heads + 2) * HEAD,
    )(h, wq, wk, wv, cos, sin)


def _first_half(o_ref, h_ref, wo_ref, ot_ref):
    o = jnp.concatenate([o_ref[n] for n in range(o_ref.shape[0])], axis=1)
    ot_ref[...] = o.T
    h1 = h_ref[...].astype(F32) + _dot(o, wo_ref[...], 1, 0).astype(BF16).astype(F32)
    return h1.astype(BF16)


def _forward_mlp(o_ref, h_ref, wo_ref, wg_ref, wu_ref, wd_ref, ot_ref, h1_ref, bt_ref, gu_ref, actt_ref, *h2_ref):
    h1 = _first_half(o_ref, h_ref, wo_ref, ot_ref)
    h1_ref[...] = h1
    b, _, _ = _normed(h1)
    bt_ref[...] = b.T
    ff = wg_ref.shape[1]
    y = jnp.zeros(h1.shape, F32)
    for at, to in _chunks(ff):
        gate = _dot(b, wg_ref[:, at:to], 1, 0)
        up = _dot(b, wu_ref[:, at:to], 1, 0)
        gu_ref[:, at:to] = gate
        gu_ref[:, ff + at : ff + to] = up
        act = (gate * _sigmoid(gate) * up).astype(BF16)
        actt_ref[at:to, :] = act.T
        if h2_ref:
            y += _dot(act, wd_ref[at:to, :], 1, 0)
    if h2_ref:
        h2_ref[0][...] = (h1.astype(F32) + y.astype(BF16).astype(F32)).astype(BF16)


def forward_mlp(number, o, h, wo, wg, wu, wd, last, tm=256):
    (heads, t, _), d, ff = o.shape, h.shape[1], wg.shape[2]
    return _call(
        _forward_mlp, "forward_mlp", (t // tm,),
        [_heads(heads, tm), _rows(tm, d), *(_layer(number, w) for w in (wo, wg, wu, wd))],
        [_columns(heads * HEAD, tm), _rows(tm, d), _columns(d, tm), _rows(tm, 2 * ff), _columns(ff, tm), _rows(tm, d)][: 5 if last else 6],
        [_like(heads * HEAD, t), _like(t, d), _like(d, t), _like(t, 2 * ff, dtype=F32), _like(ff, t), _like(t, d)][: 5 if last else 6],
        2 * t * d * (heads * HEAD + (2 if last else 3) * ff),
    )(o, h, wo, wg, wu, wd)


def _back(dy, h1, gate_up, o_ref, wo_ref, wg_ref, wu_ref, wd_ref, dgu_ref, dh1_ref, do_ref, delta_ref):
    ff = wg_ref.shape[1]
    db = jnp.zeros(dy.shape, F32)
    for at, to in _chunks(ff):
        gate, up = gate_up(at, to)
        by = _dot(dy, wd_ref[at:to, :], 1, 1).astype(BF16).astype(F32)
        s = _sigmoid(gate)
        silu = gate * s
        dup = (by * silu).astype(BF16)
        dgate = (by * up * (s + silu * (1 - s))).astype(BF16)
        dgu_ref[:, at:to] = dgate
        dgu_ref[:, ff + at : ff + to] = dup
        db += _dot(dgate, wg_ref[:, at:to], 1, 1) + _dot(dup, wu_ref[:, at:to], 1, 1)
    _, wide, scale = _normed(h1)
    dn = _normed_bwd(db.astype(BF16).astype(F32), wide, scale).astype(BF16)
    dh1 = (dy.astype(F32) + dn.astype(F32)).astype(BF16)
    dh1_ref[...] = dh1
    do = _dot(dh1, wo_ref[...], 1, 1).astype(BF16)
    for n in range(o_ref.shape[0]):
        mine = do[:, n * HEAD : (n + 1) * HEAD]
        do_ref[n] = mine
        delta_ref[n : n + 1, :] = (mine.astype(F32) * o_ref[n].astype(F32)).T.sum(0, keepdims=True)


def _backward_mlp(dy_ref, h1_ref, gu_ref, o_ref, wo_ref, wg_ref, wu_ref, wd_ref, dgu_ref, dh1_ref, do_ref, delta_ref):
    ff = wg_ref.shape[1]
    kept = lambda at, to: (gu_ref[:, at:to], gu_ref[:, ff + at : ff + to])
    _back(dy_ref[...], h1_ref[...], kept, o_ref, wo_ref, wg_ref, wu_ref, wd_ref, dgu_ref, dh1_ref, do_ref, delta_ref)


def backward_mlp(number, dy, h1, gu, o, wo, wg, wu, wd, tm=256):
    (heads, t, _), d, ff = o.shape, h1.shape[1], wg.shape[2]
    return _call(
        _backward_mlp, "backward_mlp", (t // tm,),
        [_rows(tm, d), _rows(tm, d), _rows(tm, 2 * ff), _heads(heads, tm), *(_layer(number, w) for w in (wo, wg, wu, wd))],
        [_rows(tm, 2 * ff), _rows(tm, d), _heads(heads, tm), _columns(heads, tm)],
        [_like(t, 2 * ff), _like(t, d), _like(heads, t, HEAD), _like(heads, t, dtype=F32)],
        2 * t * d * (heads * HEAD + 3 * ff),
    )(dy, h1, gu, o, wo, wg, wu, wd)


def _qkv_bwd_kernel(dq_ref, dk_ref, dv_ref, cos_ref, sin_ref, *rest):
    cos, sin = cos_ref[...], -sin_ref[...]
    parts = [_turn(dq_ref[n].astype(F32), cos, sin).astype(BF16) for n in range(dq_ref.shape[0])]
    parts += [_turn(dk_ref[...].astype(F32), cos, sin).astype(BF16), dv_ref[...]]
    dqkv_ref = rest[-1] if len(rest) == 1 else rest[-2]
    for n, part in enumerate(parts):
        dqkv_ref[:, n * HEAD : (n + 1) * HEAD] = part
    if len(rest) > 1:
        h_ref, dh1_ref, wq_ref, wk_ref, wv_ref, _, dh_ref = rest
        da = _dot(jnp.concatenate(parts[:-2], 1), wq_ref[...], 1, 1)
        da += _dot(jnp.concatenate(parts[-2:], 1), jnp.concatenate([wk_ref[...], wv_ref[...]], 1), 1, 1)
        _, wide, scale = _normed(h_ref[...])
        dn = _normed_bwd(da.astype(BF16).astype(F32), wide, scale).astype(BF16)
        dh_ref[...] = (dh1_ref[...].astype(F32) + dn.astype(F32)).astype(BF16)


def qkv_bwd(number, dq, dk, dv, cos, sin, more=None, tm=512):
    heads, t, _ = dq.shape
    width = (heads + 2) * HEAD
    ins, outs, shapes, d = [_heads(heads, tm)] + [_rows(tm, HEAD)] * 4, [_rows(tm, width)], [_like(t, width)], 1
    if more is not None:
        d = more[0].shape[1]
        ins += [_rows(tm, d), _rows(tm, d), *(_layer(number, w) for w in more[2:])]
        outs, shapes = outs + [_rows(tm, d)], shapes + [_like(t, d)]
    return _call(_qkv_bwd_kernel, "qkv_bwd", (t // tm,), ins, outs, shapes, 2 * t * d * width)(dq, dk, dv, cos, sin, *(more or ()))


def _weight_rows(left_ref, right_ref, *rest):
    out_ref = rest[-1]
    out_ref[...] = _dot(left_ref[...], right_ref[...], 1, 0).astype(BF16).reshape(out_ref.shape)


def _weight_columns(tn, left_ref, right_ref, out_ref):
    devices, r = out_ref.shape[0], left_ref.shape[0] // out_ref.shape[0]
    g = _dot(left_ref[...], right_ref[...], 1, 0).astype(BF16)
    for n in range(g.shape[1] // tn):
        out_ref[:, n * r : (n + 1) * r, :] = g[:, n * tn : (n + 1) * tn].reshape(devices, r, tn)


def weight_columns(left, right, devices, rows_all, tn, wide=640):
    (rows, t), n = left.shape, right.shape[1]
    r = rows // devices
    return pl.pallas_call(
        functools.partial(_weight_columns, tn),
        name="weight_columns",
        grid=(n // wide,),
        in_specs=[_whole((rows, t)), pl.BlockSpec((t, wide), lambda j: (0, j))],
        out_specs=pl.BlockSpec((devices, r * (wide // tn), tn), lambda j: (0, j, 0)),
        out_shape=_like(devices, rows_all, tn),
        compiler_params=pltpu.CompilerParams(dimension_semantics=("arbitrary",), vmem_limit_bytes=VMEM),
        cost_estimate=pl.CostEstimate(flops=2 * rows * t * n, bytes_accessed=2 * (rows * t + t * n + rows * n), transcendentals=0),
    )(left, right)


def weight_rows(left, right, devices, per, into=None, at=0):
    (rows, t), n = left.shape, right.shape[1]
    r = rows // devices
    given, specs, alias = [left, right], [pl.BlockSpec((per * r, t), lambda i: (i, 0)), _whole((t, n))], {}
    if into is not None:
        given, specs, alias = given + [into], specs + [ANY], {2: 0}
    return pl.pallas_call(
        _weight_rows,
        name="weight_rows",
        grid=(devices // per,),
        in_specs=specs,
        out_specs=pl.BlockSpec((pl.Element(per), pl.Element(r), pl.Element(n)), lambda i: (i * per, at, 0)) if at else pl.BlockSpec((per, r, n), lambda i: (i, 0, 0)),
        out_shape=_like(devices, r, n) if into is None else _like(*into.shape),
        input_output_aliases=alias,
        compiler_params=pltpu.CompilerParams(dimension_semantics=("arbitrary",), vmem_limit_bytes=VMEM),
        cost_estimate=pl.CostEstimate(flops=2 * rows * t * n, bytes_accessed=2 * (rows * t + t * n + rows * n), transcendentals=0),
    )(*given)


def adamw(w, m, v, g):
    m = 0.9 * m + 0.1 * g
    v = 0.95 * v + 0.05 * g * g
    step = m * lax.rsqrt(v + 1e-8) + 0.1 * w
    return (w - 0.02 * step).astype(BF16), m, v


def _adamw_kernel(rows, tn, terms, me_ref, *rest):
    k = len(rows)
    g_refs, rest = rest[:terms], rest[terms:]
    w_refs, m_refs, v_refs = (rest[i * k : (i + 1) * k] for i in range(3))
    new_ref, *outs = rest[-1 - 2 * k :]
    at = 0
    for i, r in enumerate(rows):
        for left in range(0, w_refs[i].shape[2], tn):
            here = (0, slice(None), slice(left, left + tn))
            g = g_refs[0][at : at + r, :].astype(F32)
            for ref in g_refs[1:]:
                g += ref[at : at + r, :].astype(F32)
            g = g.astype(BF16).astype(F32)
            new, m, v = adamw(w_refs[i][here].astype(F32), m_refs[i][here], v_refs[i][here], g)
            new_ref[at : at + r, :], outs[i][here], outs[k + i][here] = new, m, v
            at += r


def adamw_step(me, number, g, ws, ms, vs, before):
    terms, g = g, g[0]
    tn = g.shape[1]
    layers, rows = ms[0].shape[0], [m.shape[1] for m in ms]
    mine = lambda m: pl.BlockSpec((1, *m.shape[1:]), lambda i, me: (number, me[0], 0))
    moment = lambda m: pl.BlockSpec((1, *m.shape[1:]), lambda i, me: (number, 0, 0))
    flat = pl.BlockSpec(g.shape, lambda i, me: (0, 0))
    given = [*terms, *ws, *ms, *vs]
    specs = [*[flat] * len(terms), *map(mine, ms), *map(moment, ms), *map(moment, vs)]
    alias = {}
    if before is not None:
        alias = {1 + len(given) + i: 1 + i for i in range(len(before))}
        given += before
        specs += [ANY] * len(before)
    new, *moments = pl.pallas_call(
        functools.partial(_adamw_kernel, rows, tn, len(terms)),
        name="adamw",
        grid_spec=pltpu.PrefetchScalarGridSpec(
            num_scalar_prefetch=1, grid=(1,), in_specs=specs, out_specs=[flat, *map(moment, ms), *map(moment, vs)],
        ),
        out_shape=[_like(*g.shape)] + [_like(*m.shape, dtype=F32) for m in (*ms, *vs)],
        input_output_aliases=alias,
        compiler_params=pltpu.CompilerParams(dimension_semantics=("arbitrary",), vmem_limit_bytes=VMEM),
        cost_estimate=pl.CostEstimate(flops=20 * g.size, bytes_accessed=30 * g.size, transcendentals=g.size),
    )(me, *given)
    return new, moments


def _spread_kernel(numbers, rows, *refs):
    k = len(rows)
    all_ref, outs = refs[0], refs[-3 - k : -3]
    here, in_sem, out_sem = refs[-3:]
    devices = all_ref.shape[0]
    tn = all_ref.shape[2]
    ins = [pltpu.make_async_copy(all_ref.at[j], here.at[j], in_sem.at[j]) for j in range(devices)]
    for copy in ins:
        copy.start()
    out = []
    for j, copy in enumerate(ins):
        copy.wait()
        at = n = 0
        for number, ref, r in [(number, *one) for number in numbers for one in zip(outs, rows)]:
            for left in range(0, ref.shape[2], tn):
                target = ref.at[number, pl.ds(j * r, r), pl.ds(left, tn)]
                out.append(pltpu.make_async_copy(here.at[j, pl.ds(at, r), :], target, out_sem.at[j, n]))
                out[-1].start()
                at, n = at + r, n + 1
    for copy in out:
        copy.wait()


def spread(numbers, everyone, shapes, before):
    devices, total, tn = everyone.shape
    rows = [s[1] // devices for s in shapes]
    tiles = len(numbers) * sum(s[2] // tn for s in shapes)
    given, alias = [everyone], {}
    if before is not None:
        alias = {1 + i: i for i in range(len(before))}
        given += before
    return pl.pallas_call(
        functools.partial(_spread_kernel, numbers, rows),
        name="spread",
        in_specs=[ANY] * len(given),
        out_specs=[ANY] * len(shapes),
        out_shape=[_like(*s) for s in shapes],
        scratch_shapes=[pltpu.VMEM(everyone.shape, BF16), pltpu.SemaphoreType.DMA((devices,)), pltpu.SemaphoreType.DMA((devices, tiles))],
        input_output_aliases=alias,
        compiler_params=pltpu.CompilerParams(vmem_limit_bytes=VMEM),
        cost_estimate=pl.CostEstimate(flops=everyone.size, bytes_accessed=4 * everyone.size, transcendentals=0),
    )(*given)


def solution(mesh):
    devices = mesh.shape["dp"]
    chips = devices // 2
    rightward = [(i, (i + 2) % devices) for i in range(devices)]
    leftward = [(i, (i - 2) % devices) for i in range(devices)]
    across = [(i, i ^ 1) for i in range(devices)]
    send = lambda a, way: lax.ppermute(a, "dp", way)

    def ringed(terms):
        chip, core = lax.axis_index("dp") // 2, lax.axis_index("dp") % 2
        _, r, n = terms.shape
        terms = terms.reshape(chips, 2, r, n)
        keep = lax.dynamic_index_in_dim(terms, core, 1, False)
        got = send(lax.dynamic_index_in_dim(terms, 1 - core, 1, False), across)
        block = lambda step: [lax.dynamic_index_in_dim(a, (chip + step) % chips, 0, False) for a in (keep, got)]
        both = lambda step: sum(a.astype(F32) for a in block(step))
        cut = r // 2
        far = both(2)
        first, second = send(far[:cut].astype(BF16), rightward), send(far[cut:].astype(BF16), leftward)
        nexts, prevs = both(1), both(-1)
        nexts = jnp.concatenate([nexts[:cut] + first.astype(F32), nexts[cut:]], 0)
        prevs = jnp.concatenate([prevs[:cut], prevs[cut:] + second.astype(F32)], 0)
        return [*block(0), send(nexts.astype(BF16), rightward), send(prevs.astype(BF16), leftward)]

    def step(x, dy, *arrays):
        weights, m, v = (arrays[i : i + 7] for i in (0, 7, 14))
        wq, wk, wv, wo, wg, wu, wd = weights
        layers = wq.shape[0]
        me = jnp.reshape(lax.axis_index("dp"), (1,))
        cos, sin = _tables(x.shape[1])
        groups = {"d": (6,), "guo": (4, 5, 3), "qkv": (0, 1, 2)}
        moments = {name: None for name in groups}
        whole = {name: None for name in groups}

        summed = lambda terms: [lax.psum_scatter(terms, "dp", scatter_dimension=0, tiled=False)]
        gathered = lambda new: lax.all_gather(new, "dp", axis=0, tiled=False)
        after = lax.optimization_barrier

        def stepped(name, number, g):
            which = groups[name]
            new, moments[name] = adamw_step(me, number, g, *([s[i] for i in which] for s in (weights, m, v)), moments[name])
            return new

        def place(name, everyone, *numbers):
            whole[name] = spread(numbers, everyone, [weights[i].shape for i in groups[name]], whole[name])

        h, kept = x[0], []
        for i in range(layers):
            at, q, k, val = qkv(i, h, wq, wk, wv, cos, sin)
            o, lse = attend(q, k, val)
            ot, h1, bt, gu, actt, *result = forward_mlp(i, o, h, wo, wg, wu, wd, i == layers - 1)
            kept.append((h, at, q, k, val, o, lse, ot, h1, bt, gu, actt))
            h = result[0] if result else None
        dh = dy[0]
        behind, fresh_qkv = [], []
        for i in reversed(range(layers)):
            h, at, q, k, val, o, lse, ot, h1, bt, gu, actt = kept[i]
            by_d = weight_rows(actt, dh, devices, 1)
            gu, by_d = after((gu, by_d))
            g_d = summed(by_d)
            dgu, dh1, do, delta = backward_mlp(i, dh, h1, gu, o, wo, wg, wu, wd)
            first_one = not behind
            if first_one:
                dgu, g_d = after((dgu, g_d))
                new_d = stepped("d", i, g_d)
                dgu, new_d = after((dgu, new_d))
                all_d = gathered(new_d)
            else:
                dgu, all_guo = after((dgu, behind[0]))
                place("guo", all_guo, i + 1)
            r = sum(wo.shape[1:2] + (wg.shape[1] * wg.shape[2] // 320,)) // devices
            by_guo = weight_columns(bt, dgu, devices, r, 640)
            by_guo = weight_rows(ot, dh1, devices, devices // 2, by_guo, r - wo.shape[1] // devices)
            if first_one:
                do, by_guo, all_d = after((do, by_guo, all_d))
            else:
                do, by_guo, g_d, g_qkv = after((do, by_guo, g_d, behind[1]))
                new_d = stepped("d", i, g_d)
                fresh_qkv.append(stepped("qkv", i + 1, g_qkv))
                do, by_guo, new_d, fresh_qkv = after((do, by_guo, new_d, fresh_qkv))
            g_guo = summed(by_guo)
            dq, dk, dv = attend_bwd(q, k, val, do, lse, delta)
            dq, g_guo = after((dq, g_guo))
            new_guo = stepped("guo", i, g_guo)
            dq, new_guo = after((dq, new_guo))
            if not first_one:
                all_d = gathered(new_d)
            all_guo = gathered(new_guo)
            got = qkv_bwd(i, dq, dk, dv, cos, sin, (h, dh1, wq, wk, wv) if i else None)
            by_qkv = weight_columns(at, got[0], devices, got[0].shape[1] // HEAD * at.shape[0] // devices, HEAD)
            if i:
                dh, by_qkv = after((got[-1], by_qkv))
            elif not first_one:
                by_qkv, all_d = after((by_qkv, all_d))
            place("d", all_d, i)
            behind = [all_guo, summed(by_qkv) if i else ringed(by_qkv)]
        fresh_qkv.append(stepped("qkv", 0, behind[1]))
        all_guo, fresh_qkv = after((behind[0], fresh_qkv))
        place("guo", all_guo, 0)
        place("qkv", gathered(jnp.concatenate(fresh_qkv, 0)), *reversed(range(layers)))
        new, first, second = [None] * 7, [None] * 7, [None] * 7
        for name, which in groups.items():
            for n, i in enumerate(which):
                new[i], first[i], second[i] = whole[name][n], moments[name][n], moments[name][len(which) + n]
        return (*new, *first, *second)

    states, all_of, cut = P(("rep", "dp"), None, None), P(None, None, None), P(None, "dp", None)
    return jax.shard_map(
        step,
        mesh=mesh,
        in_specs=(states, states) + (all_of,) * 7 + (cut,) * 14,
        out_specs=(P("rep", None, None),) * 7 + (P("rep", "dp", None),) * 14,
        check_vma=False,
    )
```
